8 devices in a mesh: dp: 1 (over z), ep2: 2 (over y), ep: 4 (over x, core).
Axes of the slice: x: 2, y: 2, z: 1, core: 2. Of those that a mesh axis runs over, the one named last changes fastest.
Arguments:
- tokens: bfloat16 [1024, 1536], P(('dp', 'ep2', 'ep'))
- expert_ids: int32 [1024, 8], P(('dp', 'ep2', 'ep'))
- gates: float32 [1024, 8], P(('dp', 'ep2', 'ep'))
- w_gate: bfloat16 [40, 1536, 512], P(('ep2', 'ep'))
- w_up: bfloat16 [40, 1536, 512], P(('ep2', 'ep'))
- w_down: bfloat16 [40, 512, 1536], P(('ep2', 'ep'))
Outputs:
- output: bfloat16 [1024, 1536], P(('dp', 'ep2', 'ep'))
All inputs are finite; a program needn't handle non-finite values.
Results may differ from the reference program's by a relative error of at most 0.001.
Values are sent between devices in bfloat16 or wider.
A program may use at most 1 GiB of HBM per device.

```python
import jax
import jax.numpy as jnp
from jax import lax

MODEL_DIM = 1536
FFN_DIM = 512
NUM_EXPERTS = 40
TOP_K = 8
TOK_DEV = 128
GROUP_DEVS = 8


def random_perms(perm_key, n_rows, length):
    scores = jax.random.randint(perm_key, (n_rows, length), 0, 1048576) * length + jnp.arange(length)[None, :]
    return jnp.argsort(scores, axis=1, stable=True)


def draw_routing(route_key):
    local_count = NUM_EXPERTS // GROUP_DEVS
    key_dev, key_loc, key_tok, key_off = jax.random.split(route_key, 4)
    dev_perm = random_perms(key_dev, GROUP_DEVS, GROUP_DEVS)
    loc_perm = random_perms(key_loc, GROUP_DEVS, local_count)
    tok_perm = random_perms(key_tok, GROUP_DEVS, TOK_DEV)
    offset = jax.random.randint(key_off, (GROUP_DEVS, 1, 1), 0, NUM_EXPERTS)
    row_pos = offset + tok_perm[:, :, None] * TOP_K + jnp.arange(TOP_K)[None, None, :]
    row_mod = (row_pos % NUM_EXPERTS).reshape(GROUP_DEVS, TOK_DEV * TOP_K)
    dev_col = row_mod % GROUP_DEVS
    loc_col = row_mod // GROUP_DEVS
    dest_dev = jnp.take_along_axis(dev_perm, dev_col, axis=1)
    dest_loc = (jnp.take_along_axis(loc_perm, loc_col, axis=1) + dev_col) % local_count
    expert_ids = dest_dev * local_count + dest_loc
    return expert_ids.reshape(GROUP_DEVS * TOK_DEV, TOP_K).astype(jnp.int32)


def setup_inputs(seed: int = 0, part: int = 0) -> dict:
    base_key = jax.random.key(seed)
    part_key = jax.random.fold_in(base_key, part)
    key_x, key_route, key_gate = jax.random.split(part_key, 3)
    key_w1, key_w3, key_w2 = jax.random.split(base_key, 3)
    n_tok = GROUP_DEVS * TOK_DEV
    tokens = jax.random.normal(key_x, (n_tok, MODEL_DIM), jnp.float32).astype(jnp.bfloat16)
    expert_ids = draw_routing(key_route)
    gates = jax.nn.softmax(1.5 * jax.random.normal(key_gate, (n_tok, TOP_K), jnp.float32), axis=-1)
    w_gate = (jax.random.normal(key_w1, (NUM_EXPERTS, MODEL_DIM, FFN_DIM), jnp.float32) * MODEL_DIM ** -0.5).astype(jnp.bfloat16)
    w_up = (jax.random.normal(key_w3, (NUM_EXPERTS, MODEL_DIM, FFN_DIM), jnp.float32) * MODEL_DIM ** -0.5).astype(jnp.bfloat16)
    w_down = (jax.random.normal(key_w2, (NUM_EXPERTS, FFN_DIM, MODEL_DIM), jnp.float32) * (3.0 * FFN_DIM ** -0.5)).astype(jnp.bfloat16)
    return {'tokens': tokens, 'expert_ids': expert_ids, 'gates': gates, 'w_gate': w_gate, 'w_up': w_up, 'w_down': w_down}


def expert_rows(operands):
    rows, w_one, w_three, w_two = operands
    act_gate = jnp.dot(rows, w_one, preferred_element_type=jnp.float32)
    act_up = jnp.dot(rows, w_three, preferred_element_type=jnp.float32)
    hidden = (jax.nn.silu(act_gate) * act_up).astype(jnp.bfloat16)
    return jnp.dot(hidden, w_two, preferred_element_type=jnp.float32).astype(jnp.bfloat16)


def reference(tokens, expert_ids, gates, w_gate, w_up, w_down):
    n_tok = tokens.shape[0]
    n_rows = n_tok * TOP_K
    per_expert = GROUP_DEVS * ((TOK_DEV * TOP_K + NUM_EXPERTS - 1) // NUM_EXPERTS)
    flat_ids = expert_ids.reshape(n_rows)
    sort_order = jnp.argsort(flat_ids, stable=True)
    counts = jnp.bincount(flat_ids, length=NUM_EXPERTS)
    starts = jnp.cumsum(counts) - counts
    rank_sorted = (jnp.arange(n_rows) - starts[flat_ids[sort_order]]).astype(jnp.int32)
    row_rank = jnp.zeros((n_rows,), jnp.int32).at[sort_order].set(rank_sorted)
    dest_pos = flat_ids * per_expert + row_rank
    buffer = jnp.zeros((NUM_EXPERTS * per_expert, MODEL_DIM), tokens.dtype).at[dest_pos].set(jnp.repeat(tokens, TOP_K, axis=0))
    expert_out = lax.map(expert_rows, (buffer.reshape(NUM_EXPERTS, per_expert, MODEL_DIM), w_gate, w_up, w_down))
    picked = expert_out.reshape(NUM_EXPERTS * per_expert, MODEL_DIM)[dest_pos].reshape(n_tok, TOP_K, MODEL_DIM)
    total = tokens.astype(jnp.float32)
    for slot_j in range(TOP_K):
        total = total + gates[:, slot_j:slot_j + 1] * picked[:, slot_j].astype(jnp.float32)
    return total.astype(jnp.bfloat16)
```

```python
import jax
import jax.numpy as jnp
from jax import lax
from jax.experimental import pallas as pl
from jax.experimental.pallas import tpu as pltpu
from jax.sharding import PartitionSpec as P

MESH = pl.DeviceIdType.MESH
OWN, FIRST, DIAG, SECOND = 0, 1, 2, 3
PAD = 64
BF16_MAX = 3.3895313892515355e38


def split3(v):
    hi = jnp.minimum(v, BF16_MAX).astype(jnp.bfloat16)
    rest = v - hi.astype(jnp.float32)
    mid = rest.astype(jnp.bfloat16)
    low = (rest - mid.astype(jnp.float32)).astype(jnp.bfloat16)
    return hi, mid, low


def layer_kernel(tok_hbm, ids_hbm, gates_hbm, w1_hbm, w3_hbm, w2_hbm, out_ref,
                 xall, meta, ids_v, gates_v, w1, w3, w2, sel, gpart, xs, yb,
                 pmine, pother, qrecv, rbuf,
                 lsem, wsem, msend, mrecv, xsend, xrecv, qsem_s, qsem_r, rsend, rrecv):
    n_local, model, ffn = w1.shape
    n_tok = tok_hbm.shape[0]
    half = model // 2
    dp, y, ep = lax.axis_index("dp"), lax.axis_index("ep2"), lax.axis_index("ep")
    x, c = ep // 2, lax.rem(ep, 2)
    fx, fy = lax.rem(x + 1 - c, 2), lax.rem(y + c, 2)
    sx, sy = lax.rem(x + c, 2), lax.rem(y + 1 - c, 2)
    gx, gy = 1 - x, 1 - y

    def dev(cy, cx, core):
        return (dp, cy, cx * 2 + core)

    partner = dev(y, x, 1 - c)
    first, second, diag = dev(fy, fx, c), dev(sy, sx, c), dev(gy, gx, c)
    first_o, second_o, diag_o = dev(fy, fx, 1 - c), dev(sy, sx, 1 - c), dev(gy, gx, 1 - c)

    cx_own = pltpu.make_async_copy(tok_hbm, xall.at[OWN, 0], lsem.at[0])
    c_ids = pltpu.make_async_copy(ids_hbm, ids_v, lsem.at[1])
    c_gates = pltpu.make_async_copy(gates_hbm, gates_v, lsem.at[2])
    c_ids.start()
    c_gates.start()
    cx_own.start()

    def weight_copies(e):
        return (pltpu.make_async_copy(w1_hbm.at[e], w1.at[e], wsem.at[0, e]),
                pltpu.make_async_copy(w3_hbm.at[e], w3.at[e], wsem.at[1, e]),
                pltpu.make_async_copy(w2_hbm.at[e], w2.at[e], wsem.at[2, e]))

    for e in range(n_local):
        for cp in weight_copies(e):
            cp.start()

    barrier = pltpu.get_barrier_semaphore()
    peers = (partner, first, second, diag, first_o, second_o, diag_o)
    for peer in peers:
        pl.semaphore_signal(barrier, inc=1, device_id=peer, device_id_type=MESH)

    c_ids.wait()
    c_gates.wait()
    eye8 = (lax.broadcasted_iota(jnp.int32, (8, 8), 0)
            == lax.broadcasted_iota(jnp.int32, (8, 8), 1)).astype(jnp.float32).astype(jnp.bfloat16)

    def flip(v):
        return lax.dot_general(eye8, v, (((1,), (1,)), ((), ())), preferred_element_type=jnp.float32)

    g_hi, g_mid, g_low = split3(gates_v[...])
    meta[OWN, 0, 0:8, :] = flip(ids_v[...].astype(jnp.float32).astype(jnp.bfloat16))
    meta[OWN, 0, 8:16, :] = (flip(g_hi) + flip(g_mid)) + flip(g_low)
    yb[n_local * PAD:, :] = jnp.zeros((yb.shape[0] - n_local * PAD, model), jnp.bfloat16)

    pl.semaphore_wait(barrier, 7)

    def remote(src, dst, ssem, rsem, to):
        return pltpu.make_async_remote_copy(src_ref=src, dst_ref=dst, send_sem=ssem, recv_sem=rsem,
                                            device_id=to, device_id_type=MESH)

    meta_to = ((partner, OWN, 1), (first, FIRST, 0), (second, SECOND, 0), (diag, DIAG, 0),
               (diag_o, DIAG, 1), (second_o, SECOND, 1), (first_o, FIRST, 1))
    m_copies = [remote(meta.at[OWN, 0], meta.at[p, s], msend.at[k], mrecv.at[k], to)
                for k, (to, p, s) in enumerate(meta_to)]
    for cp in m_copies:
        cp.start()
    meta_of = {(p, s): m_copies[k] for k, (to, p, s) in enumerate(meta_to)}

    x_own_partner = remote(xall.at[OWN, 0], xall.at[OWN, 1], xsend.at[0], xrecv.at[0], partner)
    x_first = remote(xall.at[OWN, 0], xall.at[FIRST, 0], xsend.at[1], xrecv.at[1], first)
    x_second = remote(xall.at[OWN, 0], xall.at[SECOND, 0], xsend.at[2], xrecv.at[2], second)
    x_diag = remote(xall.at[FIRST, 0], xall.at[DIAG, 0], xsend.at[3], xrecv.at[3], second)
    x_fwd = {p: remote(xall.at[p, 0], xall.at[p, 1], xsend.at[3 + p], xrecv.at[3 + p], partner)
             for p in (FIRST, DIAG, SECOND)}

    cx_own.wait()
    x_first.start()
    x_own_partner.start()

    base = ((y * 4 + ep) * n_local).astype(jnp.float32)

    def route(p):
        ids = jnp.concatenate([meta[p, 0, 0:8, :], meta[p, 1, 0:8, :]], axis=1)
        gts = jnp.concatenate([meta[p, 0, 8:16, :], meta[p, 1, 8:16, :]], axis=1)
        n2 = 2 * n_tok
        chosen, gate = [], []
        for e in range(n_local):
            hit = ids == base + float(e)
            chosen.append(jnp.sum(jnp.where(hit, 1.0, 0.0), axis=0, keepdims=True))
            gate.append(jnp.sum(jnp.where(hit, gts, 0.0), axis=0, keepdims=True))
        chosen8 = jnp.concatenate(chosen + [jnp.zeros((8 - n_local, n2), jnp.float32)], axis=0)
        upper = (lax.broadcasted_iota(jnp.int32, (n2, n2), 0)
                 < lax.broadcasted_iota(jnp.int32, (n2, n2), 1)).astype(jnp.float32).astype(jnp.bfloat16)
        rank = jnp.dot(chosen8.astype(jnp.bfloat16), upper, preferred_element_type=jnp.float32)
        pos = jnp.where(chosen8 > 0.0, rank, 999.0)
        slot = lax.broadcasted_iota(jnp.int32, (PAD, n2), 0).astype(jnp.float32)
        rows = []
        for e in range(n_local):
            mask = pos[e:e + 1, :] == slot
            sel[e * PAD:(e + 1) * PAD, :] = jnp.where(mask, 1.0, 0.0).astype(jnp.bfloat16)
            rows.append(jnp.where(mask, gate[e], 0.0))
        rows.append(jnp.zeros((yb.shape[0] - n_local * PAD, n2), jnp.float32))
        spread = jnp.concatenate(rows, axis=0).T
        for k, piece in enumerate(split3(spread)):
            gpart[k] = piece

    def gather(p):
        for k in range(3):
            cols = pl.ds(k * (model // 3), model // 3)
            xg = xall[p, :, :, cols].reshape(2 * n_tok, model // 3)
            xs[:, cols] = jnp.dot(sel[...], xg, preferred_element_type=jnp.float32).astype(jnp.bfloat16)

    def ffn(fresh):
        def step(e, carry):
            if fresh:
                for cp in weight_copies(e):
                    cp.wait()
            rows = pl.ds(pl.multiple_of(e * PAD, PAD), PAD)
            xr = xs[rows, :]
            a = jnp.dot(xr, w1[e], preferred_element_type=jnp.float32)
            b = jnp.dot(xr, w3[e], preferred_element_type=jnp.float32)
            h = (jax.nn.silu(a) * b).astype(jnp.bfloat16)
            yb[rows, :] = jnp.dot(h, w2[e], preferred_element_type=jnp.float32).astype(jnp.bfloat16)
            return carry
        lax.fori_loop(0, n_local, step, 0)

    q_copies = {(p, h): remote(pother.at[p, h], qrecv.at[p, h], qsem_s.at[2 * p + h], qsem_r.at[2 * p + h], partner)
                for p in range(4) for h in range(2)}

    def combine(p):
        for h in range(2):
            ycols = yb[:, h * half:(h + 1) * half]
            acc = jnp.dot(gpart[2], ycols, preferred_element_type=jnp.float32)
            acc = acc + jnp.dot(gpart[1], ycols, preferred_element_type=jnp.float32)
            acc = acc + jnp.dot(gpart[0], ycols, preferred_element_type=jnp.float32)
            pmine[p, h] = acc[:n_tok]
            pother[p, h] = acc[n_tok:]
            q_copies[p, h].start()

    def chip_sum(p, h):
        q_copies[p, h].wait_recv()
        pmine[p, h] = pmine[p, h] + qrecv[p, h]

    r_copies = []

    def send(src, slot, rows, to):
        k = len(r_copies)
        view = slice(None) if rows is None else pl.ds(*rows)
        cp = remote(src.at[view], rbuf.at[slot].at[view], rsend.at[k], rrecv.at[k], to)
        r_copies.append(cp)
        cp.start()
        return cp

    hr = n_tok // 2

    meta_of[OWN, 1].wait_recv()
    route(OWN)
    x_own_partner.wait_recv()
    gather(OWN)
    ffn(True)
    combine(OWN)

    x_first.wait_recv()
    x_fwd[FIRST].start()
    x_diag.start()
    x_second.start()
    meta_of[FIRST, 0].wait_recv()
    meta_of[FIRST, 1].wait_recv()
    route(FIRST)
    x_fwd[FIRST].wait_recv()
    gather(FIRST)
    ffn(False)
    combine(FIRST)

    x_diag.wait_recv()
    x_fwd[DIAG].start()
    meta_of[DIAG, 0].wait_recv()
    meta_of[DIAG, 1].wait_recv()
    route(DIAG)
    chip_sum(FIRST, 0)
    to_first = send(pmine.at[FIRST, 0], 0, None, first)
    chip_sum(FIRST, 1)
    x_fwd[DIAG].wait_recv()
    gather(DIAG)
    ffn(False)
    combine(DIAG)

    x_second.wait_recv()
    x_fwd[SECOND].start()
    meta_of[SECOND, 0].wait_recv()
    meta_of[SECOND, 1].wait_recv()
    route(SECOND)
    chip_sum(DIAG, 0)
    d_first = [send(pmine.at[DIAG, 0], 2, (k * hr, hr), first) for k in range(2)]
    chip_sum(DIAG, 1)
    d_second = [send(pmine.at[DIAG, 1], 3, (k * hr, hr), second) for k in range(2)]
    x_fwd[SECOND].wait_recv()
    gather(SECOND)
    ffn(False)
    combine(SECOND)

    chip_sum(OWN, 0)
    chip_sum(OWN, 1)
    chip_sum(SECOND, 1)
    to_second = send(pmine.at[SECOND, 1], 1, None, second)
    chip_sum(SECOND, 0)

    tail = []
    for k in range(2):
        rows = pl.ds(k * hr, hr)
        d_second[k].wait_recv()
        pmine[FIRST, 1, rows, :] = pmine[FIRST, 1, rows, :] + rbuf[3, rows, :]
        tail.append(send(pmine.at[FIRST, 1], 5, (k * hr, hr), first))
        d_first[k].wait_recv()
        pmine[SECOND, 0, rows, :] = pmine[SECOND, 0, rows, :] + rbuf[2, rows, :]
        tail.append(send(pmine.at[SECOND, 0], 4, (k * hr, hr), second))

    to_first.wait_recv()
    to_second.wait_recv()
    for h in range(2):
        cols = pl.ds(h * half, half)
        pmine[OWN, h] = (pmine[OWN, h] + xall[OWN, 0, :, cols].astype(jnp.float32)) + rbuf[h]
    for k in range(2):
        rows = pl.ds(k * hr, hr)
        tail[2 * k].wait_recv()
        out_ref[rows, half:] = (pmine[OWN, 1, rows, :] + rbuf[5, rows, :]).astype(jnp.bfloat16)
        tail[2 * k + 1].wait_recv()
        out_ref[rows, :half] = (pmine[OWN, 0, rows, :] + rbuf[4, rows, :]).astype(jnp.bfloat16)

    for cp in m_copies + [x_own_partner, x_first, x_second, x_diag] + list(x_fwd.values()) + list(q_copies.values()) + r_copies:
        cp.wait_send()


def solution(mesh):
    row_spec = P(('dp', 'ep2', 'ep'), None)
    weight_spec = P(('ep2', 'ep'), None, None)

    def device_step(tokens, expert_ids, gates, w_gate, w_up, w_down):
        n_tok, model = tokens.shape
        n_local, _, ffn = w_gate.shape
        n_top = expert_ids.shape[1]
        half = model // 2
        bf16, f32 = jnp.bfloat16, jnp.float32
        dma = pltpu.SemaphoreType.DMA
        any_spec = pl.BlockSpec(memory_space=pl.ANY)
        return pl.pallas_call(
            layer_kernel,
            out_shape=jax.ShapeDtypeStruct((n_tok, model), bf16),
            in_specs=[any_spec] * 6,
            out_specs=pl.BlockSpec(memory_space=pltpu.VMEM),
            scratch_shapes=[
                pltpu.VMEM((4, 2, n_tok, model), bf16),
                pltpu.VMEM((4, 2, 16, n_tok), f32),
                pltpu.VMEM((n_tok, n_top), jnp.int32),
                pltpu.VMEM((n_tok, n_top), f32),
                pltpu.VMEM((n_local, model, ffn), bf16),
                pltpu.VMEM((n_local, model, ffn), bf16),
                pltpu.VMEM((n_local, ffn, model), bf16),
                pltpu.VMEM((n_local * PAD, 2 * n_tok), bf16),
                pltpu.VMEM((3, 2 * n_tok, 6 * PAD), bf16),
                pltpu.VMEM((n_local * PAD, model), bf16),
                pltpu.VMEM((6 * PAD, model), bf16),
                pltpu.VMEM((4, 2, n_tok, half), f32),
                pltpu.VMEM((4, 2, n_tok, half), f32),
                pltpu.VMEM((4, 2, n_tok, half), f32),
                pltpu.VMEM((6, n_tok, half), f32),
                dma((3,)),
                dma((3, n_local)),
                dma((7,)), dma((7,)),
                dma((7,)), dma((7,)),
                dma((8,)), dma((8,)),
                dma((10,)), dma((10,)),
            ],
            compiler_params=pltpu.CompilerParams(
                collective_id=0, has_side_effects=True, vmem_limit_bytes=60 * 1024 * 1024),
        )(tokens, expert_ids, gates, w_gate, w_up, w_down)

    return jax.shard_map(device_step, mesh=mesh, in_specs=(row_spec, row_spec, row_spec, weight_spec, weight_spec, weight_spec), out_specs=row_spec, check_vma=False)
```

```python
import jax
import jax.numpy as jnp
from jax import lax
from jax.experimental import pallas as pl
from jax.experimental.pallas import tpu as pltpu
from jax.sharding import PartitionSpec as P

MESH = pl.DeviceIdType.MESH
OWN, FIRST, DIAG, SECOND = 0, 1, 2, 3
PAD, RANKS = 64, 32
BF16_MAX = 3.3895313892515355e38


def split3(v):
    hi = jnp.minimum(v, BF16_MAX).astype(jnp.bfloat16)
    rest = v - hi.astype(jnp.float32)
    mid = rest.astype(jnp.bfloat16)
    low = (rest - mid.astype(jnp.float32)).astype(jnp.bfloat16)
    return hi, mid, low


def layer_kernel(tok_hbm, ids_hbm, gates_hbm, w1_hbm, w3_hbm, w2_hbm, out_hbm,
                 xall, meta, ids_v, w1, w3, w2, sel, gpart, xs, yb,
                 pmine, pother, qrecv, rbuf, out_v,
                 lsem, wsem, osem, msend, mrecv, xsend, xrecv, qsem_s, qsem_r, rsend, rrecv):
    n_local, model, ffn_dim = w1.shape
    n_tok = tok_hbm.shape[0]
    half, hr = model // 2, n_tok // 2
    dp, y, ep = lax.axis_index("dp"), lax.axis_index("ep2"), lax.axis_index("ep")
    x, c = ep // 2, lax.rem(ep, 2)
    fx, fy = lax.rem(x + 1 - c, 2), lax.rem(y + c, 2)
    sx, sy = lax.rem(x + c, 2), lax.rem(y + 1 - c, 2)

    def dev(cy, cx, core):
        return (dp, cy, cx * 2 + core)

    partner, first, second = dev(y, x, 1 - c), dev(fy, fx, c), dev(sy, sx, c)

    c_ids = pltpu.make_async_copy(ids_hbm, ids_v, lsem.at[1])
    c_gates = pltpu.make_async_copy(gates_hbm, meta.at[OWN, 0, pl.ds(8, 8)], lsem.at[2])
    c_own = pltpu.make_async_copy(tok_hbm, xall.at[OWN, 0], lsem.at[0])
    c_ids.start()
    c_gates.start()
    c_own.start()

    barrier = pltpu.get_barrier_semaphore()
    for peer in (partner, first, second):
        pl.semaphore_signal(barrier, inc=1, device_id=peer, device_id_type=MESH)

    def weight_copies(e):
        return (pltpu.make_async_copy(w1_hbm.at[e], w1.at[e], wsem.at[0, e]),
                pltpu.make_async_copy(w3_hbm.at[e], w3.at[e], wsem.at[1, e]),
                pltpu.make_async_copy(w2_hbm.at[e], w2.at[e], wsem.at[2, e]))

    for e in range(n_local):
        for cp in weight_copies(e):
            cp.start()

    c_ids.wait()
    meta[OWN, 0, 0:8, :] = ids_v[...].astype(jnp.float32)
    c_gates.wait()
    c_own.wait()

    def remote(src, dst, ssem, rsem, to):
        return pltpu.make_async_remote_copy(src_ref=src, dst_ref=dst, send_sem=ssem, recv_sem=rsem,
                                            device_id=to, device_id_type=MESH)

    hops = ((OWN, OWN, 1, partner), (OWN, FIRST, 0, first), (OWN, SECOND, 0, second), (FIRST, DIAG, 0, second),
            (FIRST, FIRST, 1, partner), (DIAG, DIAG, 1, partner), (SECOND, SECOND, 1, partner))
    m_hop = [remote(meta.at[s, 0], meta.at[p, q], msend.at[k], mrecv.at[k], to)
             for k, (s, p, q, to) in enumerate(hops)]
    x_hop = {k: remote(xall.at[s, 0], xall.at[p, q], xsend.at[k], xrecv.at[k], to)
             for k, (s, p, q, to) in enumerate(hops) if k != 2}
    second_cut = [remote(xall.at[OWN, 0, pl.ds(k * hr, hr)], xall.at[SECOND, 0, pl.ds(k * hr, hr)],
                         xsend.at[(2, 7)[k]], xrecv.at[(2, 7)[k]], second) for k in range(2)]

    pl.semaphore_wait(barrier, 3)
    m_hop[1].start()
    x_hop[1].start()
    m_hop[0].start()
    x_hop[0].start()
    m_hop[2].start()
    yb[:, :, n_local * RANKS:, :] = jnp.zeros((2, 2, yb.shape[2] - n_local * RANKS, model), jnp.bfloat16)

    base = ((y * 4 + ep) * n_local).astype(jnp.float32)

    def route(p, b):
        n2 = 2 * n_tok
        ids = jnp.concatenate([meta[p, 0, 0:8, :], meta[p, 1, 0:8, :]], axis=1)
        gts = jnp.concatenate([meta[p, 0, 8:16, :], meta[p, 1, 8:16, :]], axis=1)
        chosen, gate = [], []
        for e in range(n_local):
            hit = ids == base + float(e)
            chosen.append(jnp.sum(jnp.where(hit, 1.0, 0.0), axis=0, keepdims=True))
            gate.append(jnp.sum(jnp.where(hit, gts, 0.0), axis=0, keepdims=True))
        chosen8 = jnp.concatenate(chosen + [jnp.zeros((8 - n_local, n2), jnp.float32)], axis=0)
        row, col = lax.broadcasted_iota(jnp.int32, (n2, n2), 0), lax.broadcasted_iota(jnp.int32, (n2, n2), 1)
        earlier = ((row < col) & ((row < n_tok) == (col < n_tok))).astype(jnp.float32).astype(jnp.bfloat16)
        rank = jnp.dot(chosen8.astype(jnp.bfloat16), earlier, preferred_element_type=jnp.float32)
        pos = jnp.where(chosen8 > 0.0, rank, 999.0)
        slot = lax.broadcasted_iota(jnp.int32, (RANKS, n_tok), 0).astype(jnp.float32)
        none = jnp.zeros((RANKS, n_tok), jnp.bfloat16)
        for q in range(2):
            lanes = slice(q * n_tok, (q + 1) * n_tok)
            rows = []
            for e in range(n_local):
                mask = pos[e:e + 1, lanes] == slot
                at = e * PAD + q * RANKS
                sel[at:at + RANKS, lanes] = jnp.where(mask, 1.0, 0.0).astype(jnp.bfloat16)
                sel[at:at + RANKS, (1 - q) * n_tok:(2 - q) * n_tok] = none
                rows.append(jnp.where(mask, gate[e][:, lanes], 0.0))
            rows.append(jnp.zeros((yb.shape[2] - n_local * RANKS, n_tok), jnp.float32))
            spread = jnp.concatenate(rows, axis=0).T
            for k, piece in enumerate(split3(spread)):
                gpart[b, q, k] = piece

    def gather(p):
        for k in range(3):
            cols = pl.ds(k * (model // 3), model // 3)
            xg = xall[p, :, :, cols].reshape(2 * n_tok, model // 3)
            xs[:, cols] = jnp.dot(sel[...], xg, preferred_element_type=jnp.float32).astype(jnp.bfloat16)

    def ffn(b, fresh=False, hooks={}):
        for e in range(n_local):
            for hook in hooks.get(e, ()):
                hook()
            if fresh:
                for cp in weight_copies(e):
                    cp.wait()
            xr = xs[e * PAD:(e + 1) * PAD, :]
            up = jnp.dot(xr, w1[e], preferred_element_type=jnp.float32)
            lin = jnp.dot(xr, w3[e], preferred_element_type=jnp.float32)
            h = (jax.nn.silu(up) * lin).astype(jnp.bfloat16)
            yr = jnp.dot(h, w2[e], preferred_element_type=jnp.float32).astype(jnp.bfloat16)
            for q in range(2):
                yb[b, q, e * RANKS:(e + 1) * RANKS, :] = yr[q * RANKS:(q + 1) * RANKS]

    q_copies = {(p, h): remote(pother.at[p, h], qrecv.at[p, h], qsem_s.at[2 * p + h], qsem_r.at[2 * p + h], partner)
                for p in range(4) for h in range(2)}

    def combine(p, b, h):
        for q in (1, 0):
            ycols = yb[b, q, :, h * half:(h + 1) * half]
            acc = jnp.dot(gpart[b, q, 2], ycols, preferred_element_type=jnp.float32)
            acc = acc + jnp.dot(gpart[b, q, 1], ycols, preferred_element_type=jnp.float32)
            acc = acc + jnp.dot(gpart[b, q, 0], ycols, preferred_element_type=jnp.float32)
            if q == 1:
                pother[p, h] = acc
                q_copies[p, h].start()
            else:
                pmine[p, h] = acc

    def chip_sum(p, h):
        q_copies[p, h].wait_recv()
        pmine[p, h] = pmine[p, h] + qrecv[p, h]

    returns = {"to_first": (FIRST, 0, 0, first), "to_second": (SECOND, 1, 1, second),
               "diag_first": (DIAG, 0, 2, first), "diag_second": (DIAG, 1, 3, second),
               "last_second": (SECOND, 0, 4, second), "last_first": (FIRST, 1, 5, first)}
    ret = {name: [remote(pmine.at[p, h, pl.ds(k * hr, hr)], rbuf.at[slot, pl.ds(k * hr, hr)],
                         rsend.at[slot, k], rrecv.at[slot, k], to) for k in range(2)]
           for name, (p, h, slot, to) in returns.items()}

    def start_both(name):
        for cp in ret[name]:
            cp.start()

    def sum_and_send(p, h, name):
        def run():
            chip_sum(p, h)
            start_both(name)
        return run

    def on_first_sent():
        x_hop[1].wait_send()
        second_cut[0].start()

    def on_first():
        m_hop[1].wait_recv()
        m_hop[4].start()
        m_hop[3].start()
        x_hop[1].wait_recv()
        x_hop[4].start()
        x_hop[3].start()
        second_cut[1].start()

    def on_diag():
        m_hop[3].wait_recv()
        m_hop[5].start()
        x_hop[3].wait_recv()
        x_hop[5].start()

    def on_second():
        m_hop[2].wait_recv()
        m_hop[6].start()
        for cp in second_cut:
            cp.wait_recv()
        x_hop[6].start()

    m_hop[0].wait_recv()
    route(OWN, 1)
    x_hop[0].wait_recv()
    gather(OWN)
    ffn(1, True, {3: (on_first_sent,), 4: (on_first,)})

    m_hop[4].wait_recv()
    route(FIRST, 0)
    x_hop[4].wait_recv()
    gather(FIRST)
    ffn(0)
    combine(FIRST, 0, 0)
    on_diag()
    combine(FIRST, 0, 1)

    m_hop[5].wait_recv()
    route(DIAG, 0)
    sum_and_send(FIRST, 0, "to_first")()
    x_hop[5].wait_recv()
    gather(DIAG)
    ffn(0, False, {1: (on_second,), 2: (lambda: chip_sum(FIRST, 1),)})
    combine(DIAG, 0, 0)
    combine(DIAG, 0, 1)

    m_hop[6].wait_recv()
    route(SECOND, 0)
    x_hop[6].wait_recv()
    gather(SECOND)
    ffn(0, False, {1: (sum_and_send(DIAG, 0, "diag_first"),), 2: (sum_and_send(DIAG, 1, "diag_second"),)})
    combine(SECOND, 0, 1)
    combine(SECOND, 0, 0)
    combine(OWN, 1, 0)
    sum_and_send(SECOND, 1, "to_second")()
    combine(OWN, 1, 1)
    chip_sum(SECOND, 0)

    for k in range(2):
        rows = pl.ds(k * hr, hr)
        ret["diag_second"][k].wait_recv()
        pmine[FIRST, 1, rows, :] = pmine[FIRST, 1, rows, :] + rbuf[3, rows, :]
        ret["last_first"][k].start()
        ret["diag_first"][k].wait_recv()
        pmine[SECOND, 0, rows, :] = pmine[SECOND, 0, rows, :] + rbuf[2, rows, :]
        ret["last_second"][k].start()
    chip_sum(OWN, 0)
    chip_sum(OWN, 1)
    for h, name in ((0, "to_first"), (1, "to_second")):
        for cp in ret[name]:
            cp.wait_recv()
        cols = pl.ds(h * half, half)
        pmine[OWN, h] = (pmine[OWN, h] + xall[OWN, 0, :, cols].astype(jnp.float32)) + rbuf[h]
    outs = []
    for k in range(2):
        rows = pl.ds(k * hr, hr)
        ret["last_first"][k].wait_recv()
        out_v[rows, half:] = (pmine[OWN, 1, rows, :] + rbuf[5, rows, :]).astype(jnp.bfloat16)
        ret["last_second"][k].wait_recv()
        out_v[rows, :half] = (pmine[OWN, 0, rows, :] + rbuf[4, rows, :]).astype(jnp.bfloat16)
        outs.append(pltpu.make_async_copy(out_v.at[rows], out_hbm.at[rows], osem.at[k]))
        outs[-1].start()

    for cp in m_hop + [x_hop[k] for k in (0, 3, 4, 5, 6)] + second_cut + list(q_copies.values()):
        cp.wait_send()
    for pair in ret.values():
        for cp in pair:
            cp.wait_send()
    for cp in outs:
        cp.wait()


def solution(mesh):
    row_spec = P(('dp', 'ep2', 'ep'), None)
    weight_spec = P(('ep2', 'ep'), None, None)

    def device_step(tokens, expert_ids, gates, w_gate, w_up, w_down):
        n_tok, model = tokens.shape
        n_local, _, ffn = w_gate.shape
        n_top = expert_ids.shape[1]
        half = model // 2
        bf16, f32 = jnp.bfloat16, jnp.float32
        dma = pltpu.SemaphoreType.DMA
        any_spec = pl.BlockSpec(memory_space=pl.ANY)
        return pl.pallas_call(
            layer_kernel,
            out_shape=jax.ShapeDtypeStruct((n_tok, model), bf16),
            in_specs=[any_spec] * 6,
            out_specs=any_spec,
            scratch_shapes=[
                pltpu.VMEM((4, 2, n_tok, model), bf16),
                pltpu.VMEM((4, 2, 16, n_tok), f32),
                pltpu.VMEM((n_top, n_tok), jnp.int32),
                pltpu.VMEM((n_local, model, ffn), bf16),
                pltpu.VMEM((n_local, model, ffn), bf16),
                pltpu.VMEM((n_local, ffn, model), bf16),
                pltpu.VMEM((n_local * PAD, 2 * n_tok), bf16),
                pltpu.VMEM((2, 2, 3, n_tok, 8 * RANKS), bf16),
                pltpu.VMEM((n_local * PAD, model), bf16),
                pltpu.VMEM((2, 2, 8 * RANKS, model), bf16),
                pltpu.VMEM((4, 2, n_tok, half), f32),
                pltpu.VMEM((4, 2, n_tok, half), f32),
                pltpu.VMEM((4, 2, n_tok, half), f32),
                pltpu.VMEM((6, n_tok, half), f32),
                pltpu.VMEM((n_tok, model), bf16),
                dma((3,)), dma((3, n_local)), dma((2,)),
                dma((7,)), dma((7,)),
                dma((8,)), dma((8,)),
                dma((8,)), dma((8,)),
                dma((6, 2)), dma((6, 2)),
            ],
            compiler_params=pltpu.CompilerParams(
                collective_id=0, has_side_effects=True, vmem_limit_bytes=60 * 1024 * 1024),
        )(tokens, expert_ids.T, gates.T, w_gate, w_up, w_down)

    return jax.shard_map(device_step, mesh=mesh, in_specs=(row_spec, row_spec, row_spec, weight_spec, weight_spec, weight_spec), out_specs=row_spec, check_vma=False)
```

```python
import jax
import jax.numpy as jnp
from jax import lax
from jax.experimental import pallas as pl
from jax.experimental.pallas import tpu as pltpu
from jax.sharding import PartitionSpec as P

MESH = pl.DeviceIdType.MESH
OWN, FIRST, DIAG, SECOND = 0, 1, 2, 3
PAD, RANKS, CUTS = 64, 32, 4
BF16_MAX = 3.3895313892515355e38


def split3(v):
    hi = jnp.minimum(v, BF16_MAX).astype(jnp.bfloat16)
    rest = v - hi.astype(jnp.float32)
    mid = rest.astype(jnp.bfloat16)
    low = (rest - mid.astype(jnp.float32)).astype(jnp.bfloat16)
    return hi, mid, low


def layer_kernel(tok_hbm, ids_hbm, gates_hbm, w1_hbm, w3_hbm, w2_hbm, out_hbm,
                 xall, meta, ids_v, w1, w3, w2, sel, gpart, xs, yb,
                 pmine, pother, qrecv, rbuf, out_v,
                 lsem, wsem, osem, msend, mrecv, xsend, xrecv, qsem_s, qsem_r, rsend, rrecv):
    n_local, model, ffn_dim = w1.shape
    n_tok = tok_hbm.shape[0]
    half, hr = model // 2, n_tok // 2
    dp, y, ep = lax.axis_index("dp"), lax.axis_index("ep2"), lax.axis_index("ep")
    x, c = ep // 2, lax.rem(ep, 2)
    fx, fy = lax.rem(x + 1 - c, 2), lax.rem(y + c, 2)
    sx, sy = lax.rem(x + c, 2), lax.rem(y + 1 - c, 2)

    def dev(cy, cx, core):
        return (dp, cy, cx * 2 + core)

    partner, first, second = dev(y, x, 1 - c), dev(fy, fx, c), dev(sy, sx, c)

    c_ids = pltpu.make_async_copy(ids_hbm, ids_v, lsem.at[1])
    c_gates = pltpu.make_async_copy(gates_hbm, meta.at[OWN, 0, pl.ds(8, 8)], lsem.at[2])
    c_own = pltpu.make_async_copy(tok_hbm, xall.at[OWN, 0], lsem.at[0])
    c_ids.start()
    c_gates.start()
    c_own.start()

    barrier = pltpu.get_barrier_semaphore()
    for peer in (partner, first, second):
        pl.semaphore_signal(barrier, inc=1, device_id=peer, device_id_type=MESH)

    def weight_copies(e):
        return (pltpu.make_async_copy(w1_hbm.at[e], w1.at[e], wsem.at[0, e]),
                pltpu.make_async_copy(w3_hbm.at[e], w3.at[e], wsem.at[1, e]),
                pltpu.make_async_copy(w2_hbm.at[e], w2.at[e], wsem.at[2, e]))

    for e in range(n_local):
        for cp in weight_copies(e):
            cp.start()

    c_ids.wait()
    meta[OWN, 0, 0:8, :] = ids_v[...].astype(jnp.float32)
    c_gates.wait()
    c_own.wait()

    def remote(src, dst, ssem, rsem, to):
        return pltpu.make_async_remote_copy(src_ref=src, dst_ref=dst, send_sem=ssem, recv_sem=rsem,
                                            device_id=to, device_id_type=MESH)

    hops = ((OWN, OWN, 1, partner), (OWN, FIRST, 0, first), (OWN, SECOND, 0, second), (FIRST, DIAG, 0, second),
            (FIRST, FIRST, 1, partner), (DIAG, DIAG, 1, partner), (SECOND, SECOND, 1, partner))
    m_hop = [remote(meta.at[s, 0], meta.at[p, q], msend.at[k], mrecv.at[k], to)
             for k, (s, p, q, to) in enumerate(hops)]
    cut = n_tok // CUTS
    x_hop = [[remote(xall.at[s, 0, pl.ds(i * cut, cut)], xall.at[p, q, pl.ds(i * cut, cut)],
                     xsend.at[k, i], xrecv.at[k, i], to) for i in range(CUTS)]
             for k, (s, p, q, to) in enumerate(hops)]

    def start_x(k):
        for cp in x_hop[k]:
            cp.start()

    def wait_x(k):
        for cp in x_hop[k]:
            cp.wait_recv()

    pl.semaphore_wait(barrier, 3)
    m_hop[1].start()
    start_x(1)
    m_hop[0].start()
    start_x(0)
    m_hop[2].start()
    xs[n_local * PAD:, :] = jnp.zeros((PAD, model), jnp.bfloat16)
    yb[:, :, n_local * RANKS:, :] = jnp.zeros((2, 2, yb.shape[2] - n_local * RANKS, model), jnp.bfloat16)

    base = ((y * 4 + ep) * n_local).astype(jnp.float32)

    def route(p, b):
        n2 = 2 * n_tok
        ids = jnp.concatenate([meta[p, 0, 0:8, :], meta[p, 1, 0:8, :]], axis=1)
        gts = jnp.concatenate([meta[p, 0, 8:16, :], meta[p, 1, 8:16, :]], axis=1)
        chosen, gate = [], []
        for e in range(n_local):
            hit = ids == base + float(e)
            chosen.append(jnp.sum(jnp.where(hit, 1.0, 0.0), axis=0, keepdims=True))
            gate.append(jnp.sum(jnp.where(hit, gts, 0.0), axis=0, keepdims=True))
        chosen8 = jnp.concatenate(chosen + [jnp.zeros((8 - n_local, n2), jnp.float32)], axis=0)
        row, col = lax.broadcasted_iota(jnp.int32, (n2, n2), 0), lax.broadcasted_iota(jnp.int32, (n2, n2), 1)
        earlier = ((row < col) & ((row < n_tok) == (col < n_tok))).astype(jnp.float32).astype(jnp.bfloat16)
        rank = jnp.dot(chosen8.astype(jnp.bfloat16), earlier, preferred_element_type=jnp.float32)
        pos = jnp.where(chosen8 > 0.0, rank, 999.0)
        slot = lax.broadcasted_iota(jnp.int32, (RANKS, n_tok), 0).astype(jnp.float32)
        none = jnp.zeros((RANKS, n_tok), jnp.bfloat16)
        for q in range(2):
            lanes = slice(q * n_tok, (q + 1) * n_tok)
            rows = []
            for e in range(n_local):
                mask = pos[e:e + 1, lanes] == slot
                at = e * PAD + q * RANKS
                sel[at:at + RANKS, lanes] = jnp.where(mask, 1.0, 0.0).astype(jnp.bfloat16)
                sel[at:at + RANKS, (1 - q) * n_tok:(2 - q) * n_tok] = none
                rows.append(jnp.where(mask, gate[e][:, lanes], 0.0))
            rows.append(jnp.zeros((yb.shape[2] - n_local * RANKS, n_tok), jnp.float32))
            spread = jnp.concatenate(rows, axis=0).T
            for k, piece in enumerate(split3(spread)):
                gpart[b, q, k] = piece

    def gather(p):
        for k in range(3):
            cols = pl.ds(k * (model // 3), model // 3)
            xg = xall[p, :, :, cols].reshape(2 * n_tok, model // 3)
            xs[:n_local * PAD, cols] = jnp.dot(sel[...], xg, preferred_element_type=jnp.float32).astype(jnp.bfloat16)

    def up(e):
        xr = xs[e * PAD:e * PAD + 2 * PAD, :]
        act = jnp.dot(xr, w1[e], preferred_element_type=jnp.float32)
        lin = jnp.dot(xr, w3[e], preferred_element_type=jnp.float32)
        return (jax.nn.silu(act) * lin).astype(jnp.bfloat16)

    def down(e, b, h):
        yr = jnp.dot(h, w2[e], preferred_element_type=jnp.float32)
        for q in range(2):
            yb[b, q, e * RANKS:(e + 1) * RANKS, :] = yr[q * RANKS:(q + 1) * RANKS].astype(jnp.bfloat16)

    def ffn(b, fresh=False, hooks={}):
        def ready(e):
            if fresh:
                for cp in weight_copies(e):
                    cp.wait()
            return up(e)

        h = None if fresh else up(0)
        for e in range(n_local):
            if fresh:
                h, ahead = ready(e), None
            else:
                ahead = up(e + 1) if e + 1 < n_local else None
            down(e, b, h)
            h = ahead
            for hook in hooks.get(e, ()):
                hook()

    q_copies = {(p, h): remote(pother.at[p, h], qrecv.at[p, h], qsem_s.at[2 * p + h], qsem_r.at[2 * p + h], partner)
                for p in range(4) for h in range(2)}

    def combine(p, b, h):
        for q in (1, 0):
            ycols = yb[b, q, :, h * half:(h + 1) * half]
            acc = jnp.dot(gpart[b, q, 2], ycols, preferred_element_type=jnp.float32)
            acc = acc + jnp.dot(gpart[b, q, 1], ycols, preferred_element_type=jnp.float32)
            acc = acc + jnp.dot(gpart[b, q, 0], ycols, preferred_element_type=jnp.float32)
            if q == 1:
                pother[p, h] = acc
                q_copies[p, h].start()
            else:
                pmine[p, h] = acc

    def chip_sum(p, h):
        q_copies[p, h].wait_recv()
        pmine[p, h] = pmine[p, h] + qrecv[p, h]

    returns = {"to_first": (FIRST, 0, 0, first), "to_second": (SECOND, 1, 1, second),
               "diag_first": (DIAG, 0, 2, first), "diag_second": (DIAG, 1, 3, second),
               "last_second": (SECOND, 0, 4, second), "last_first": (FIRST, 1, 5, first)}
    ret = {name: [remote(pmine.at[p, h, pl.ds(k * hr, hr)], rbuf.at[slot, pl.ds(k * hr, hr)],
                         rsend.at[slot, k], rrecv.at[slot, k], to) for k in range(2)]
           for name, (p, h, slot, to) in returns.items()}

    def start_both(name):
        for cp in ret[name]:
            cp.start()

    def sum_and_send(p, h, name):
        def run():
            chip_sum(p, h)
            start_both(name)
        return run

    def on_first(i):
        if i == 0:
            m_hop[1].wait_recv()
            m_hop[4].start()
            m_hop[3].start()
        x_hop[1][i].wait_recv()
        x_hop[3][i].start()
        x_hop[4][i].start()

    def on_diag(i):
        if i == 0:
            m_hop[3].wait_recv()
            m_hop[5].start()
        x_hop[3][i].wait_recv()
        x_hop[5][i].start()

    def on_second():
        m_hop[2].wait_recv()
        m_hop[6].start()
        wait_x(2)
        start_x(6)

    def after_three():
        on_first(2)
        m_hop[4].wait_recv()
        route(FIRST, 0)
        on_first(3)
        start_x(2)

    m_hop[0].wait_recv()
    route(OWN, 1)
    wait_x(0)
    gather(OWN)
    ffn(1, True, {1: (lambda: on_first(0),), 2: (lambda: on_first(1),), 3: (after_three,)})

    wait_x(4)
    gather(FIRST)
    ffn(0, False, {3: (lambda: on_diag(0), lambda: on_diag(1), lambda: on_diag(2)), 4: (lambda: on_diag(3),)})
    combine(FIRST, 0, 0)
    combine(FIRST, 0, 1)

    m_hop[5].wait_recv()
    route(DIAG, 0)
    wait_x(5)
    gather(DIAG)
    ffn(0, False, {0: (sum_and_send(FIRST, 0, "to_first"),), 2: (lambda: chip_sum(FIRST, 1),), 3: (on_second,)})
    combine(DIAG, 0, 0)
    combine(DIAG, 0, 1)

    m_hop[6].wait_recv()
    route(SECOND, 0)
    wait_x(6)
    gather(SECOND)
    ffn(0, False, {0: (sum_and_send(DIAG, 0, "diag_first"),), 1: (sum_and_send(DIAG, 1, "diag_second"),),
                   })
    combine(SECOND, 0, 1)
    combine(SECOND, 0, 0)
    combine(OWN, 1, 0)
    sum_and_send(SECOND, 1, "to_second")()
    combine(OWN, 1, 1)
    chip_sum(SECOND, 0)

    for k in range(2):
        rows = pl.ds(k * hr, hr)
        ret["diag_second"][k].wait_recv()
        pmine[FIRST, 1, rows, :] = pmine[FIRST, 1, rows, :] + rbuf[3, rows, :]
        ret["last_first"][k].start()
        ret["diag_first"][k].wait_recv()
        pmine[SECOND, 0, rows, :] = pmine[SECOND, 0, rows, :] + rbuf[2, rows, :]
        ret["last_second"][k].start()
    chip_sum(OWN, 0)
    chip_sum(OWN, 1)
    for h, name in ((0, "to_first"), (1, "to_second")):
        for cp in ret[name]:
            cp.wait_recv()
        cols = pl.ds(h * half, half)
        pmine[OWN, h] = (pmine[OWN, h] + xall[OWN, 0, :, cols].astype(jnp.float32)) + rbuf[h]
    outs = []
    for k in range(2):
        rows = pl.ds(k * hr, hr)
        ret["last_first"][k].wait_recv()
        out_v[rows, half:] = (pmine[OWN, 1, rows, :] + rbuf[5, rows, :]).astype(jnp.bfloat16)
        ret["last_second"][k].wait_recv()
        out_v[rows, :half] = (pmine[OWN, 0, rows, :] + rbuf[4, rows, :]).astype(jnp.bfloat16)
        outs.append(pltpu.make_async_copy(out_v.at[rows], out_hbm.at[rows], osem.at[k]))
        outs[-1].start()

    for cp in m_hop + [cp for pair in x_hop for cp in pair] + list(q_copies.values()):
        cp.wait_send()
    for pair in ret.values():
        for cp in pair:
            cp.wait_send()
    for cp in outs:
        cp.wait()


def solution(mesh):
    row_spec = P(('dp', 'ep2', 'ep'), None)
    weight_spec = P(('ep2', 'ep'), None, None)

    def device_step(tokens, expert_ids, gates, w_gate, w_up, w_down):
        n_tok, model = tokens.shape
        n_local, _, ffn = w_gate.shape
        n_top = expert_ids.shape[1]
        half = model // 2
        bf16, f32 = jnp.bfloat16, jnp.float32
        dma = pltpu.SemaphoreType.DMA
        any_spec = pl.BlockSpec(memory_space=pl.ANY)
        return pl.pallas_call(
            layer_kernel,
            out_shape=jax.ShapeDtypeStruct((n_tok, model), bf16),
            in_specs=[any_spec] * 6,
            out_specs=any_spec,
            scratch_shapes=[
                pltpu.VMEM((4, 2, n_tok, model), bf16),
                pltpu.VMEM((4, 2, 16, n_tok), f32),
                pltpu.VMEM((n_top, n_tok), jnp.int32),
                pltpu.VMEM((n_local, model, ffn), bf16),
                pltpu.VMEM((n_local, model, ffn), bf16),
                pltpu.VMEM((n_local, ffn, model), bf16),
                pltpu.VMEM((n_local * PAD, 2 * n_tok), bf16),
                pltpu.VMEM((2, 2, 3, n_tok, 8 * RANKS), bf16),
                pltpu.VMEM(((n_local + 1) * PAD, model), bf16),
                pltpu.VMEM((2, 2, 8 * RANKS, model), bf16),
                pltpu.VMEM((4, 2, n_tok, half), f32),
                pltpu.VMEM((4, 2, n_tok, half), f32),
                pltpu.VMEM((4, 2, n_tok, half), f32),
                pltpu.VMEM((6, n_tok, half), f32),
                pltpu.VMEM((n_tok, model), bf16),
                dma((3,)), dma((3, n_local)), dma((2,)),
                dma((7,)), dma((7,)),
                dma((7, CUTS)), dma((7, CUTS)),
                dma((8,)), dma((8,)),
                dma((6, 2)), dma((6, 2)),
            ],
            compiler_params=pltpu.CompilerParams(
                collective_id=0, has_side_effects=True, vmem_limit_bytes=60 * 1024 * 1024),
        )(tokens, expert_ids.T, gates.T, w_gate, w_up, w_down)

    return jax.shard_map(device_step, mesh=mesh, in_specs=(row_spec, row_spec, row_spec, weight_spec, weight_spec, weight_spec), out_specs=row_spec, check_vma=False)
```

```python
import jax
import jax.numpy as jnp
from jax import lax
from jax.experimental import pallas as pl
from jax.experimental.pallas import tpu as pltpu
from jax.sharding import PartitionSpec as P

MESH = pl.DeviceIdType.MESH
OWN, FIRST, DIAG, SECOND = 0, 1, 2, 3
PAD, RANKS, CUTS = 64, 32, 4
BF16_MAX = 3.3895313892515355e38


def split3(v):
    hi = jnp.minimum(v, BF16_MAX).astype(jnp.bfloat16)
    rest = v - hi.astype(jnp.float32)
    mid = rest.astype(jnp.bfloat16)
    low = (rest - mid.astype(jnp.float32)).astype(jnp.bfloat16)
    return hi, mid, low


def layer_kernel(tok_hbm, ids_hbm, gates_hbm, w1_hbm, w3_hbm, w2_hbm, out_ref,
                 xall, meta, ids_v, w1, w3, w2, sel, gpart, xs, yb,
                 pmine, pother, qrecv, rbuf,
                 lsem, wsem, msend, mrecv, xsend, xrecv, qsem_s, qsem_r, rsend, rrecv):
    n_local, model, ffn_dim = w1.shape
    n_tok = tok_hbm.shape[0]
    half, hr = model // 2, n_tok // 2
    dp, y, ep = lax.axis_index("dp"), lax.axis_index("ep2"), lax.axis_index("ep")
    x, c = ep // 2, lax.rem(ep, 2)
    fx, fy = lax.rem(x + 1 - c, 2), lax.rem(y + c, 2)
    sx, sy = lax.rem(x + c, 2), lax.rem(y + 1 - c, 2)

    def dev(cy, cx, core):
        return (dp, cy, cx * 2 + core)

    partner, first, second = dev(y, x, 1 - c), dev(fy, fx, c), dev(sy, sx, c)

    c_ids = pltpu.make_async_copy(ids_hbm, ids_v, lsem.at[1])
    c_gates = pltpu.make_async_copy(gates_hbm, meta.at[OWN, 0, pl.ds(8, 8)], lsem.at[2])
    c_own = pltpu.make_async_copy(tok_hbm, xall.at[OWN, 0], lsem.at[0])
    c_ids.start()
    c_gates.start()
    c_own.start()

    barrier = pltpu.get_barrier_semaphore()
    for peer in (partner, first, second):
        pl.semaphore_signal(barrier, inc=1, device_id=peer, device_id_type=MESH)

    def weight_copies(e):
        return (pltpu.make_async_copy(w1_hbm.at[e], w1.at[e], wsem.at[0, e]),
                pltpu.make_async_copy(w3_hbm.at[e], w3.at[e], wsem.at[1, e]),
                pltpu.make_async_copy(w2_hbm.at[e], w2.at[e], wsem.at[2, e]))

    for e in range(n_local):
        for cp in weight_copies(e):
            cp.start()

    c_ids.wait()
    meta[OWN, 0, 0:8, :] = ids_v[...].astype(jnp.float32)
    c_gates.wait()
    c_own.wait()

    def remote(src, dst, ssem, rsem, to):
        return pltpu.make_async_remote_copy(src_ref=src, dst_ref=dst, send_sem=ssem, recv_sem=rsem,
                                            device_id=to, device_id_type=MESH)

    hops = ((OWN, OWN, 1, partner), (OWN, FIRST, 0, first), (OWN, SECOND, 0, second), (FIRST, DIAG, 0, second),
            (FIRST, FIRST, 1, partner), (DIAG, DIAG, 1, partner), (SECOND, SECOND, 1, partner))
    m_hop = [remote(meta.at[s, 0], meta.at[p, q], msend.at[k], mrecv.at[k], to)
             for k, (s, p, q, to) in enumerate(hops)]
    cut = n_tok // CUTS
    x_hop = [[remote(xall.at[s, 0, pl.ds(i * cut, cut)], xall.at[p, q, pl.ds(i * cut, cut)],
                     xsend.at[k, i], xrecv.at[k, i], to) for i in range(CUTS)]
             for k, (s, p, q, to) in enumerate(hops)]

    def start_x(k):
        for cp in x_hop[k]:
            cp.start()

    def wait_x(k):
        for cp in x_hop[k]:
            cp.wait_recv()

    pl.semaphore_wait(barrier, 3)
    m_hop[1].start()
    start_x(1)
    m_hop[0].start()
    start_x(0)
    m_hop[2].start()
    xs[n_local * PAD:, :] = jnp.zeros((PAD, model), jnp.bfloat16)
    yb[:, :, n_local * RANKS:, :] = jnp.zeros((2, 2, yb.shape[2] - n_local * RANKS, model), jnp.bfloat16)

    base = ((y * 4 + ep) * n_local).astype(jnp.float32)

    def route(p, b):
        n2 = 2 * n_tok
        ids = jnp.concatenate([meta[p, 0, 0:8, :], meta[p, 1, 0:8, :]], axis=1)
        gts = jnp.concatenate([meta[p, 0, 8:16, :], meta[p, 1, 8:16, :]], axis=1)
        chosen, gate = [], []
        for e in range(n_local):
            hit = ids == base + float(e)
            chosen.append(jnp.sum(jnp.where(hit, 1.0, 0.0), axis=0, keepdims=True))
            gate.append(jnp.sum(jnp.where(hit, gts, 0.0), axis=0, keepdims=True))
        chosen8 = jnp.concatenate(chosen + [jnp.zeros((8 - n_local, n2), jnp.float32)], axis=0)
        row, col = lax.broadcasted_iota(jnp.int32, (n2, n2), 0), lax.broadcasted_iota(jnp.int32, (n2, n2), 1)
        earlier = ((row < col) & ((row < n_tok) == (col < n_tok))).astype(jnp.float32).astype(jnp.bfloat16)
        rank = jnp.dot(chosen8.astype(jnp.bfloat16), earlier, preferred_element_type=jnp.float32)
        pos = jnp.where(chosen8 > 0.0, rank, 999.0)
        slot = lax.broadcasted_iota(jnp.int32, (RANKS, n_tok), 0).astype(jnp.float32)
        none = jnp.zeros((RANKS, n_tok), jnp.bfloat16)
        for q in range(2):
            lanes = slice(q * n_tok, (q + 1) * n_tok)
            rows = []
            for e in range(n_local):
                mask = pos[e:e + 1, lanes] == slot
                at = e * PAD + q * RANKS
                sel[at:at + RANKS, lanes] = jnp.where(mask, 1.0, 0.0).astype(jnp.bfloat16)
                sel[at:at + RANKS, (1 - q) * n_tok:(2 - q) * n_tok] = none
                rows.append(jnp.where(mask, gate[e][:, lanes], 0.0))
            rows.append(jnp.zeros((yb.shape[2] - n_local * RANKS, n_tok), jnp.float32))
            spread = jnp.concatenate(rows, axis=0).T
            for k, piece in enumerate(split3(spread)):
                gpart[b, q, k] = piece

    def gather(p):
        for k in range(3):
            cols = pl.ds(k * (model // 3), model // 3)
            xg = xall[p, :, :, cols].reshape(2 * n_tok, model // 3)
            xs[:n_local * PAD, cols] = jnp.dot(sel[...], xg, preferred_element_type=jnp.float32).astype(jnp.bfloat16)

    def up(e):
        xr = xs[e * PAD:e * PAD + 2 * PAD, :]
        act = jnp.dot(xr, w1[e], preferred_element_type=jnp.float32)
        lin = jnp.dot(xr, w3[e], preferred_element_type=jnp.float32)
        return (jax.nn.silu(act) * lin).astype(jnp.bfloat16)

    def down(e, b, h):
        yr = jnp.dot(h, w2[e], preferred_element_type=jnp.float32)
        for q in range(2):
            yb[b, q, e * RANKS:(e + 1) * RANKS, :] = yr[q * RANKS:(q + 1) * RANKS].astype(jnp.bfloat16)

    def ffn(b, fresh=False, hooks={}):
        def ready(e):
            if fresh:
                for cp in weight_copies(e):
                    cp.wait()
            return up(e)

        h = None if fresh else up(0)
        for e in range(n_local):
            if fresh:
                h, ahead = ready(e), None
            else:
                ahead = up(e + 1) if e + 1 < n_local else None
            down(e, b, h)
            h = ahead
            for hook in hooks.get(e, ()):
                hook()

    q_copies = {(p, h): remote(pother.at[p, h], qrecv.at[p, h], qsem_s.at[2 * p + h], qsem_r.at[2 * p + h], partner)
                for p in range(4) for h in range(2)}

    def combine(p, b, h):
        for q in (1, 0):
            ycols = yb[b, q, :, h * half:(h + 1) * half]
            acc = jnp.dot(gpart[b, q, 2], ycols, preferred_element_type=jnp.float32)
            acc = acc + jnp.dot(gpart[b, q, 1], ycols, preferred_element_type=jnp.float32)
            acc = acc + jnp.dot(gpart[b, q, 0], ycols, preferred_element_type=jnp.float32)
            if q == 1:
                pother[p, h] = acc
                q_copies[p, h].start()
            else:
                pmine[p, h] = acc

    def chip_sum(p, h):
        q_copies[p, h].wait_recv()
        pmine[p, h] = pmine[p, h] + qrecv[p, h]

    returns = {"to_first": (FIRST, 0, 0, first), "to_second": (SECOND, 1, 1, second),
               "diag_first": (DIAG, 0, 2, first), "diag_second": (DIAG, 1, 3, second),
               "last_second": (SECOND, 0, 4, second), "last_first": (FIRST, 1, 5, first)}
    ret = {name: [remote(pmine.at[p, h, pl.ds(k * hr, hr)], rbuf.at[slot, pl.ds(k * hr, hr)],
                         rsend.at[slot, k], rrecv.at[slot, k], to) for k in range(2)]
           for name, (p, h, slot, to) in returns.items()}

    def start_both(name):
        for cp in ret[name]:
            cp.start()

    def sum_and_send(p, h, name):
        def run():
            chip_sum(p, h)
            start_both(name)
        return run

    def on_first(i):
        if i == 0:
            m_hop[1].wait_recv()
            m_hop[4].start()
            m_hop[3].start()
        x_hop[1][i].wait_recv()
        x_hop[3][i].start()
        x_hop[4][i].start()

    def on_diag(i):
        if i == 0:
            m_hop[3].wait_recv()
            m_hop[5].start()
        x_hop[3][i].wait_recv()
        x_hop[5][i].start()

    def on_second():
        m_hop[2].wait_recv()
        m_hop[6].start()
        wait_x(2)
        start_x(6)

    def after_three():
        on_first(2)
        m_hop[4].wait_recv()
        route(FIRST, 0)
        on_first(3)
        start_x(2)

    m_hop[0].wait_recv()
    route(OWN, 1)
    wait_x(0)
    gather(OWN)
    ffn(1, True, {1: (lambda: on_first(0),), 2: (lambda: on_first(1),), 3: (after_three,)})

    wait_x(4)
    gather(FIRST)
    ffn(0, False, {3: (lambda: on_diag(0), lambda: on_diag(1), lambda: on_diag(2)), 4: (lambda: on_diag(3),)})
    combine(FIRST, 0, 0)
    combine(FIRST, 0, 1)

    m_hop[5].wait_recv()
    route(DIAG, 0)
    wait_x(5)
    gather(DIAG)
    ffn(0, False, {0: (sum_and_send(FIRST, 0, "to_first"),), 2: (lambda: chip_sum(FIRST, 1),)})
    combine(DIAG, 0, 0)
    combine(DIAG, 0, 1)

    on_second()
    m_hop[6].wait_recv()
    route(SECOND, 0)
    sum_and_send(DIAG, 0, "diag_first")()
    sum_and_send(DIAG, 1, "diag_second")()
    wait_x(6)
    gather(SECOND)
    ffn(0)
    combine(SECOND, 0, 1)
    combine(SECOND, 0, 0)
    combine(OWN, 1, 0)
    sum_and_send(SECOND, 1, "to_second")()
    combine(OWN, 1, 1)
    chip_sum(SECOND, 0)

    for k in range(2):
        rows = pl.ds(k * hr, hr)
        ret["diag_second"][k].wait_recv()
        pmine[FIRST, 1, rows, :] = pmine[FIRST, 1, rows, :] + rbuf[3, rows, :]
        ret["last_first"][k].start()
        ret["diag_first"][k].wait_recv()
        pmine[SECOND, 0, rows, :] = pmine[SECOND, 0, rows, :] + rbuf[2, rows, :]
        ret["last_second"][k].start()
    chip_sum(OWN, 0)
    chip_sum(OWN, 1)
    for h, name in ((0, "to_first"), (1, "to_second")):
        for cp in ret[name]:
            cp.wait_recv()
        cols = pl.ds(h * half, half)
        pmine[OWN, h] = (pmine[OWN, h] + xall[OWN, 0, :, cols].astype(jnp.float32)) + rbuf[h]
    for k in range(2):
        rows = pl.ds(k * hr, hr)
        ret["last_first"][k].wait_recv()
        out_ref[rows, half:] = (pmine[OWN, 1, rows, :] + rbuf[5, rows, :]).astype(jnp.bfloat16)
        ret["last_second"][k].wait_recv()
        out_ref[rows, :half] = (pmine[OWN, 0, rows, :] + rbuf[4, rows, :]).astype(jnp.bfloat16)
    for cp in m_hop + [cp for pair in x_hop for cp in pair] + list(q_copies.values()):
        cp.wait_send()
    for pair in ret.values():
        for cp in pair:
            cp.wait_send()


def solution(mesh):
    row_spec = P(('dp', 'ep2', 'ep'), None)
    weight_spec = P(('ep2', 'ep'), None, None)

    def device_step(tokens, expert_ids, gates, w_gate, w_up, w_down):
        n_tok, model = tokens.shape
        n_local, _, ffn = w_gate.shape
        n_top = expert_ids.shape[1]
        half = model // 2
        bf16, f32 = jnp.bfloat16, jnp.float32
        dma = pltpu.SemaphoreType.DMA
        any_spec = pl.BlockSpec(memory_space=pl.ANY)
        return pl.pallas_call(
            layer_kernel,
            out_shape=pltpu.MemorySpace.VMEM((n_tok, model), bf16),
            in_specs=[any_spec] * 6,
            out_specs=pl.BlockSpec(memory_space=pltpu.VMEM),
            scratch_shapes=[
                pltpu.VMEM((4, 2, n_tok, model), bf16),
                pltpu.VMEM((4, 2, 16, n_tok), f32),
                pltpu.VMEM((n_top, n_tok), jnp.int32),
                pltpu.VMEM((n_local, model, ffn), bf16),
                pltpu.VMEM((n_local, model, ffn), bf16),
                pltpu.VMEM((n_local, ffn, model), bf16),
                pltpu.VMEM((n_local * PAD, 2 * n_tok), bf16),
                pltpu.VMEM((2, 2, 3, n_tok, 8 * RANKS), bf16),
                pltpu.VMEM(((n_local + 1) * PAD, model), bf16),
                pltpu.VMEM((2, 2, 8 * RANKS, model), bf16),
                pltpu.VMEM((4, 2, n_tok, half), f32),
                pltpu.VMEM((4, 2, n_tok, half), f32),
                pltpu.VMEM((4, 2, n_tok, half), f32),
                pltpu.VMEM((6, n_tok, half), f32),
                dma((3,)), dma((3, n_local)),
                dma((7,)), dma((7,)),
                dma((7, CUTS)), dma((7, CUTS)),
                dma((8,)), dma((8,)),
                dma((6, 2)), dma((6, 2)),
            ],
            compiler_params=pltpu.CompilerParams(
                collective_id=0, has_side_effects=True, vmem_limit_bytes=60 * 1024 * 1024),
        )(tokens, expert_ids.T, gates.T, w_gate, w_up, w_down)

    return jax.shard_map(device_step, mesh=mesh, in_specs=(row_spec, row_spec, row_spec, weight_spec, weight_spec, weight_spec), out_specs=row_spec, check_vma=False)
```

```python
import jax
import jax.numpy as jnp
from jax import lax
from jax.experimental import pallas as pl
from jax.experimental.pallas import tpu as pltpu
from jax.sharding import PartitionSpec as P

MESH = pl.DeviceIdType.MESH
OWN, FIRST, DIAG, SECOND = 0, 1, 2, 3
PAD, RANKS, CUTS = 64, 32, 4
BF16_MAX = 3.3895313892515355e38


def split3(v):
    hi = jnp.minimum(v, BF16_MAX).astype(jnp.bfloat16)
    rest = v - hi.astype(jnp.float32)
    mid = rest.astype(jnp.bfloat16)
    low = (rest - mid.astype(jnp.float32)).astype(jnp.bfloat16)
    return hi, mid, low


def layer_kernel(tok_hbm, ids_hbm, gates_hbm, w1_hbm, w3_hbm, w2_hbm, out_ref,
                 xall, meta, ids_v, w1, w3, w2, sel, gpart, xs, yb,
                 pmine, pother, qrecv, rbuf,
                 lsem, wsem, msend, mrecv, xsend, xrecv, qsem_s, qsem_r, rsend, rrecv):
    n_local, model, ffn_dim = w1.shape
    n_tok = tok_hbm.shape[0]
    half, hr = model // 2, n_tok // 2
    dp, y, ep = lax.axis_index("dp"), lax.axis_index("ep2"), lax.axis_index("ep")
    x, c = ep // 2, lax.rem(ep, 2)
    fx, fy = lax.rem(x + 1 - c, 2), lax.rem(y + c, 2)
    sx, sy = lax.rem(x + c, 2), lax.rem(y + 1 - c, 2)

    def dev(cy, cx, core):
        return (dp, cy, cx * 2 + core)

    partner, first, second = dev(y, x, 1 - c), dev(fy, fx, c), dev(sy, sx, c)

    c_ids = pltpu.make_async_copy(ids_hbm, ids_v, lsem.at[1])
    c_gates = pltpu.make_async_copy(gates_hbm, meta.at[OWN, 0, pl.ds(8, 8)], lsem.at[2])
    c_own = pltpu.make_async_copy(tok_hbm, xall.at[OWN, 0], lsem.at[0])
    c_ids.start()
    c_gates.start()
    c_own.start()

    barrier = pltpu.get_barrier_semaphore()
    for peer in (partner, first, second):
        pl.semaphore_signal(barrier, inc=1, device_id=peer, device_id_type=MESH)

    def weight_copies(e):
        return (pltpu.make_async_copy(w1_hbm.at[e], w1.at[e], wsem.at[0, e]),
                pltpu.make_async_copy(w3_hbm.at[e], w3.at[e], wsem.at[1, e]),
                pltpu.make_async_copy(w2_hbm.at[e], w2.at[e], wsem.at[2, e]))

    for e in range(n_local):
        for cp in weight_copies(e):
            cp.start()

    c_ids.wait()
    meta[OWN, 0, 0:8, :] = ids_v[...].astype(jnp.float32)
    c_gates.wait()
    c_own.wait()

    def remote(src, dst, ssem, rsem, to):
        return pltpu.make_async_remote_copy(src_ref=src, dst_ref=dst, send_sem=ssem, recv_sem=rsem,
                                            device_id=to, device_id_type=MESH)

    hops = ((OWN, OWN, 1, partner), (OWN, FIRST, 0, first), (OWN, SECOND, 0, second), (FIRST, DIAG, 0, second),
            (FIRST, FIRST, 1, partner), (DIAG, DIAG, 1, partner), (SECOND, SECOND, 1, partner))
    m_hop = [remote(meta.at[s, 0], meta.at[p, q], msend.at[k], mrecv.at[k], to)
             for k, (s, p, q, to) in enumerate(hops)]
    cut = n_tok // CUTS
    x_hop = [[remote(xall.at[s, 0, pl.ds(i * cut, cut)], xall.at[p, q, pl.ds(i * cut, cut)],
                     xsend.at[k, i], xrecv.at[k, i], to) for i in range(CUTS)]
             for k, (s, p, q, to) in enumerate(hops)]

    def start_x(k):
        for cp in x_hop[k]:
            cp.start()

    def wait_x(k):
        for cp in x_hop[k]:
            cp.wait_recv()

    pl.semaphore_wait(barrier, 3)
    m_hop[1].start()
    start_x(1)
    m_hop[0].start()
    start_x(0)
    m_hop[2].start()
    xs[n_local * PAD:, :] = jnp.zeros((PAD, model), jnp.bfloat16)
    yb[:, :, n_local * RANKS:, :] = jnp.zeros((2, 2, yb.shape[2] - n_local * RANKS, model), jnp.bfloat16)

    base = ((y * 4 + ep) * n_local).astype(jnp.float32)

    def route(p, b):
        n2 = 2 * n_tok
        ids = jnp.concatenate([meta[p, 0, 0:8, :], meta[p, 1, 0:8, :]], axis=1)
        gts = jnp.concatenate([meta[p, 0, 8:16, :], meta[p, 1, 8:16, :]], axis=1)
        chosen, gate = [], []
        for e in range(n_local):
            hit = ids == base + float(e)
            chosen.append(jnp.sum(jnp.where(hit, 1.0, 0.0), axis=0, keepdims=True))
            gate.append(jnp.sum(jnp.where(hit, gts, 0.0), axis=0, keepdims=True))
        chosen8 = jnp.concatenate(chosen + [jnp.zeros((8 - n_local, n2), jnp.float32)], axis=0)
        row, col = lax.broadcasted_iota(jnp.int32, (n2, n2), 0), lax.broadcasted_iota(jnp.int32, (n2, n2), 1)
        earlier = ((row < col) & ((row < n_tok) == (col < n_tok))).astype(jnp.float32).astype(jnp.bfloat16)
        rank = jnp.dot(chosen8.astype(jnp.bfloat16), earlier, preferred_element_type=jnp.float32)
        pos = jnp.where(chosen8 > 0.0, rank, 999.0)
        slot = lax.broadcasted_iota(jnp.int32, (RANKS, n_tok), 0).astype(jnp.float32)
        none = jnp.zeros((RANKS, n_tok), jnp.bfloat16)
        for q in range(2):
            lanes = slice(q * n_tok, (q + 1) * n_tok)
            rows = []
            for e in range(n_local):
                mask = pos[e:e + 1, lanes] == slot
                at = e * PAD + q * RANKS
                sel[at:at + RANKS, lanes] = jnp.where(mask, 1.0, 0.0).astype(jnp.bfloat16)
                sel[at:at + RANKS, (1 - q) * n_tok:(2 - q) * n_tok] = none
                rows.append(jnp.where(mask, gate[e][:, lanes], 0.0))
            rows.append(jnp.zeros((yb.shape[2] - n_local * RANKS, n_tok), jnp.float32))
            spread = jnp.concatenate(rows, axis=0).T
            for k, piece in enumerate(split3(spread)):
                gpart[b, q, k] = piece

    def gather(p):
        for k in range(3):
            cols = pl.ds(k * (model // 3), model // 3)
            xg = xall[p, :, :, cols].reshape(2 * n_tok, model // 3)
            xs[:n_local * PAD, cols] = jnp.dot(sel[...], xg, preferred_element_type=jnp.float32).astype(jnp.bfloat16)

    def up(e):
        xr = xs[e * PAD:e * PAD + 2 * PAD, :]
        act = jnp.dot(xr, w1[e], preferred_element_type=jnp.float32)
        lin = jnp.dot(xr, w3[e], preferred_element_type=jnp.float32)
        return (jax.nn.silu(act) * lin).astype(jnp.bfloat16)

    def down(e, b, h):
        yr = jnp.dot(h, w2[e], preferred_element_type=jnp.float32)
        for q in range(2):
            yb[b, q, e * RANKS:(e + 1) * RANKS, :] = yr[q * RANKS:(q + 1) * RANKS].astype(jnp.bfloat16)

    def ffn(b, fresh=False, hooks={}):
        def ready(e):
            if fresh:
                for cp in weight_copies(e):
                    cp.wait()
            return up(e)

        h = None if fresh else up(0)
        for e in range(n_local):
            if fresh:
                h, ahead = ready(e), None
            else:
                ahead = up(e + 1) if e + 1 < n_local else None
            down(e, b, h)
            h = ahead
            for hook in hooks.get(e, ()):
                hook()

    q_copies = {(p, h): remote(pother.at[p, h], qrecv.at[p, h], qsem_s.at[2 * p + h], qsem_r.at[2 * p + h], partner)
                for p in range(4) for h in range(2)}

    def combine(p, b, h):
        for q in (1, 0):
            ycols = yb[b, q, :, h * half:(h + 1) * half]
            acc = jnp.dot(gpart[b, q, 2], ycols, preferred_element_type=jnp.float32)
            acc = acc + jnp.dot(gpart[b, q, 1], ycols, preferred_element_type=jnp.float32)
            acc = acc + jnp.dot(gpart[b, q, 0], ycols, preferred_element_type=jnp.float32)
            if q == 1:
                pother[p, h] = acc
                q_copies[p, h].start()
            else:
                pmine[p, h] = acc

    def chip_sum(p, h):
        q_copies[p, h].wait_recv()
        pmine[p, h] = pmine[p, h] + qrecv[p, h]

    returns = {"to_first": (FIRST, 0, 0, first), "to_second": (SECOND, 1, 1, second),
               "diag_first": (DIAG, 0, 2, first), "diag_second": (DIAG, 1, 3, second),
               "last_second": (SECOND, 0, 4, second), "last_first": (FIRST, 1, 5, first)}
    ret = {name: [remote(pmine.at[p, h, pl.ds(k * hr, hr)], rbuf.at[slot, pl.ds(k * hr, hr)],
                         rsend.at[slot, k], rrecv.at[slot, k], to) for k in range(2)]
           for name, (p, h, slot, to) in returns.items()}

    def start_both(name):
        for cp in ret[name]:
            cp.start()

    def sum_and_send(p, h, name):
        def run():
            chip_sum(p, h)
            start_both(name)
        return run

    def on_first(i):
        if i == 0:
            m_hop[1].wait_recv()
            m_hop[4].start()
            m_hop[3].start()
        x_hop[1][i].wait_recv()
        x_hop[4][i].start()
        if i < CUTS - 1:
            @pl.when(c == 0)
            def _():
                x_hop[3][i].start()
        if i > 0:
            @pl.when(c == 1)
            def _():
                x_hop[3][i - 1].start()
        if i == CUTS - 1:
            x_hop[3][i].start()

    def on_diag(i):
        if i == 0:
            m_hop[3].wait_recv()
            m_hop[5].start()
        x_hop[3][i].wait_recv()
        x_hop[5][i].start()

    def on_second():
        m_hop[2].wait_recv()
        m_hop[6].start()
        wait_x(2)
        start_x(6)

    def after_three():
        on_first(2)
        m_hop[4].wait_recv()
        route(FIRST, 0)
        on_first(3)
        start_x(2)

    m_hop[0].wait_recv()
    route(OWN, 1)
    wait_x(0)
    gather(OWN)
    ffn(1, True, {1: (lambda: on_first(0),), 2: (lambda: on_first(1),), 3: (after_three,)})

    wait_x(4)
    gather(FIRST)
    ffn(0, False, {2: (lambda: on_diag(0), lambda: on_diag(1),), 3: (lambda: on_diag(2), lambda: on_diag(3),)})
    combine(FIRST, 0, 0)
    combine(FIRST, 0, 1)

    m_hop[5].wait_recv()
    route(DIAG, 0)
    wait_x(5)
    gather(DIAG)
    ffn(0, False, {0: (sum_and_send(FIRST, 0, "to_first"),), 2: (lambda: chip_sum(FIRST, 1),)})
    combine(DIAG, 0, 0)
    combine(DIAG, 0, 1)

    on_second()
    m_hop[6].wait_recv()
    route(SECOND, 0)
    sum_and_send(DIAG, 0, "diag_first")()
    sum_and_send(DIAG, 1, "diag_second")()
    wait_x(6)
    gather(SECOND)
    ffn(0)
    combine(SECOND, 0, 1)
    combine(SECOND, 0, 0)
    combine(OWN, 1, 0)
    sum_and_send(SECOND, 1, "to_second")()
    combine(OWN, 1, 1)
    chip_sum(SECOND, 0)

    for k in range(2):
        rows = pl.ds(k * hr, hr)
        ret["diag_second"][k].wait_recv()
        pmine[FIRST, 1, rows, :] = pmine[FIRST, 1, rows, :] + rbuf[3, rows, :]
        ret["last_first"][k].start()
        ret["diag_first"][k].wait_recv()
        pmine[SECOND, 0, rows, :] = pmine[SECOND, 0, rows, :] + rbuf[2, rows, :]
        ret["last_second"][k].start()
    chip_sum(OWN, 0)
    chip_sum(OWN, 1)
    for h, name in ((0, "to_first"), (1, "to_second")):
        for cp in ret[name]:
            cp.wait_recv()
        cols = pl.ds(h * half, half)
        pmine[OWN, h] = (pmine[OWN, h] + xall[OWN, 0, :, cols].astype(jnp.float32)) + rbuf[h]
    for k in range(2):
        rows = pl.ds(k * hr, hr)
        ret["last_first"][k].wait_recv()
        out_ref[rows, half:] = (pmine[OWN, 1, rows, :] + rbuf[5, rows, :]).astype(jnp.bfloat16)
        ret["last_second"][k].wait_recv()
        out_ref[rows, :half] = (pmine[OWN, 0, rows, :] + rbuf[4, rows, :]).astype(jnp.bfloat16)
    for cp in m_hop + [cp for pair in x_hop for cp in pair] + list(q_copies.values()):
        cp.wait_send()
    for pair in ret.values():
        for cp in pair:
            cp.wait_send()


def solution(mesh):
    row_spec = P(('dp', 'ep2', 'ep'), None)
    weight_spec = P(('ep2', 'ep'), None, None)

    def device_step(tokens, expert_ids, gates, w_gate, w_up, w_down):
        n_tok, model = tokens.shape
        n_local, _, ffn = w_gate.shape
        n_top = expert_ids.shape[1]
        half = model // 2
        bf16, f32 = jnp.bfloat16, jnp.float32
        dma = pltpu.SemaphoreType.DMA
        any_spec = pl.BlockSpec(memory_space=pl.ANY)
        return pl.pallas_call(
            layer_kernel,
            out_shape=pltpu.MemorySpace.VMEM((n_tok, model), bf16),
            in_specs=[any_spec] * 6,
            out_specs=pl.BlockSpec(memory_space=pltpu.VMEM),
            scratch_shapes=[
                pltpu.VMEM((4, 2, n_tok, model), bf16),
                pltpu.VMEM((4, 2, 16, n_tok), f32),
                pltpu.VMEM((n_top, n_tok), jnp.int32),
                pltpu.VMEM((n_local, model, ffn), bf16),
                pltpu.VMEM((n_local, model, ffn), bf16),
                pltpu.VMEM((n_local, ffn, model), bf16),
                pltpu.VMEM((n_local * PAD, 2 * n_tok), bf16),
                pltpu.VMEM((2, 2, 3, n_tok, 8 * RANKS), bf16),
                pltpu.VMEM(((n_local + 1) * PAD, model), bf16),
                pltpu.VMEM((2, 2, 8 * RANKS, model), bf16),
                pltpu.VMEM((4, 2, n_tok, half), f32),
                pltpu.VMEM((4, 2, n_tok, half), f32),
                pltpu.VMEM((4, 2, n_tok, half), f32),
                pltpu.VMEM((6, n_tok, half), f32),
                dma((3,)), dma((3, n_local)),
                dma((7,)), dma((7,)),
                dma((7, CUTS)), dma((7, CUTS)),
                dma((8,)), dma((8,)),
                dma((6, 2)), dma((6, 2)),
            ],
            compiler_params=pltpu.CompilerParams(
                collective_id=0, has_side_effects=True, vmem_limit_bytes=60 * 1024 * 1024),
        )(tokens, expert_ids.T, gates.T, w_gate, w_up, w_down)

    return jax.shard_map(device_step, mesh=mesh, in_specs=(row_spec, row_spec, row_spec, weight_spec, weight_spec, weight_spec), out_specs=row_spec, check_vma=False)
```

```python
import jax
import jax.numpy as jnp
from jax import lax
from jax.experimental import pallas as pl
from jax.experimental.pallas import tpu as pltpu
from jax.sharding import PartitionSpec as P

MESH = pl.DeviceIdType.MESH
OWN, FIRST, DIAG, SECOND = 0, 1, 2, 3
PAD, RANKS, CUTS = 64, 32, 4
BF16_MAX = 3.3895313892515355e38


def split3(v):
    hi = jnp.minimum(v, BF16_MAX).astype(jnp.bfloat16)
    rest = v - hi.astype(jnp.float32)
    mid = rest.astype(jnp.bfloat16)
    low = (rest - mid.astype(jnp.float32)).astype(jnp.bfloat16)
    return hi, mid, low


def layer_kernel(tok_hbm, ids_hbm, gates_hbm, w1_hbm, w3_hbm, w2_hbm, out_ref,
                 xall, meta, ids_v, w1, w3, w2, sel, gpart, xs, yb,
                 pmine, pother, qrecv, rbuf,
                 lsem, wsem, msend, mrecv, xsend, xrecv, qsem_s, qsem_r, rsend, rrecv):
    n_local, model, ffn_dim = w1.shape
    n_tok = tok_hbm.shape[0]
    half, hr = model // 2, n_tok // 2
    dp, y, ep = lax.axis_index("dp"), lax.axis_index("ep2"), lax.axis_index("ep")
    x, c = ep // 2, lax.rem(ep, 2)
    fx, fy = lax.rem(x + 1 - c, 2), lax.rem(y + c, 2)
    sx, sy = lax.rem(x + c, 2), lax.rem(y + 1 - c, 2)

    def dev(cy, cx, core):
        return (dp, cy, cx * 2 + core)

    partner, first, second = dev(y, x, 1 - c), dev(fy, fx, c), dev(sy, sx, c)

    c_ids = pltpu.make_async_copy(ids_hbm, ids_v, lsem.at[1])
    c_gates = pltpu.make_async_copy(gates_hbm, meta.at[OWN, 0, pl.ds(8, 8)], lsem.at[2])
    c_own = pltpu.make_async_copy(tok_hbm, xall.at[OWN, 0], lsem.at[0])
    c_ids.start()
    c_gates.start()
    c_own.start()

    barrier = pltpu.get_barrier_semaphore()
    for peer in (partner, first, second):
        pl.semaphore_signal(barrier, inc=1, device_id=peer, device_id_type=MESH)

    def weight_copies(e):
        return (pltpu.make_async_copy(w1_hbm.at[e], w1.at[e], wsem.at[0, e]),
                pltpu.make_async_copy(w3_hbm.at[e], w3.at[e], wsem.at[1, e]),
                pltpu.make_async_copy(w2_hbm.at[e], w2.at[e], wsem.at[2, e]))

    for e in range(n_local):
        for cp in weight_copies(e):
            cp.start()

    c_ids.wait()
    meta[OWN, 0, 0:8, :] = ids_v[...].astype(jnp.float32)
    c_gates.wait()
    c_own.wait()

    def remote(src, dst, ssem, rsem, to):
        return pltpu.make_async_remote_copy(src_ref=src, dst_ref=dst, send_sem=ssem, recv_sem=rsem,
                                            device_id=to, device_id_type=MESH)

    hops = ((OWN, OWN, 1, partner), (OWN, FIRST, 0, first), (OWN, SECOND, 0, second), (FIRST, DIAG, 0, second),
            (FIRST, FIRST, 1, partner), (DIAG, DIAG, 1, partner), (SECOND, SECOND, 1, partner))
    m_hop = [remote(meta.at[s, 0], meta.at[p, q], msend.at[k], mrecv.at[k], to)
             for k, (s, p, q, to) in enumerate(hops)]
    cut = n_tok // CUTS
    x_hop = [[remote(xall.at[s, 0, pl.ds(i * cut, cut)], xall.at[p, q, pl.ds(i * cut, cut)],
                     xsend.at[k, i], xrecv.at[k, i], to) for i in range(CUTS)]
             for k, (s, p, q, to) in enumerate(hops)]

    def start_x(k):
        for cp in x_hop[k]:
            cp.start()

    def wait_x(k):
        for cp in x_hop[k]:
            cp.wait_recv()

    pl.semaphore_wait(barrier, 3)
    m_hop[1].start()
    start_x(1)
    m_hop[0].start()
    start_x(0)
    m_hop[2].start()
    xs[n_local * PAD:, :] = jnp.zeros((PAD, model), jnp.bfloat16)
    yb[:, :, n_local * RANKS:, :] = jnp.zeros((3, 2, yb.shape[2] - n_local * RANKS, model), jnp.bfloat16)

    base = ((y * 4 + ep) * n_local).astype(jnp.float32)

    def route(p, b):
        n2 = 2 * n_tok
        ids = jnp.concatenate([meta[p, 0, 0:8, :], meta[p, 1, 0:8, :]], axis=1)
        gts = jnp.concatenate([meta[p, 0, 8:16, :], meta[p, 1, 8:16, :]], axis=1)
        chosen, gate = [], []
        for e in range(n_local):
            hit = ids == base + float(e)
            chosen.append(jnp.sum(jnp.where(hit, 1.0, 0.0), axis=0, keepdims=True))
            gate.append(jnp.sum(jnp.where(hit, gts, 0.0), axis=0, keepdims=True))
        chosen8 = jnp.concatenate(chosen + [jnp.zeros((8 - n_local, n2), jnp.float32)], axis=0)
        row, col = lax.broadcasted_iota(jnp.int32, (n2, n2), 0), lax.broadcasted_iota(jnp.int32, (n2, n2), 1)
        earlier = ((row < col) & ((row < n_tok) == (col < n_tok))).astype(jnp.float32).astype(jnp.bfloat16)
        rank = jnp.dot(chosen8.astype(jnp.bfloat16), earlier, preferred_element_type=jnp.float32)
        pos = jnp.where(chosen8 > 0.0, rank, 999.0)
        slot = lax.broadcasted_iota(jnp.int32, (RANKS, n_tok), 0).astype(jnp.float32)
        none = jnp.zeros((RANKS, n_tok), jnp.bfloat16)
        for q in range(2):
            lanes = slice(q * n_tok, (q + 1) * n_tok)
            rows = []
            for e in range(n_local):
                mask = pos[e:e + 1, lanes] == slot
                at = e * PAD + q * RANKS
                sel[at:at + RANKS, lanes] = jnp.where(mask, 1.0, 0.0).astype(jnp.bfloat16)
                sel[at:at + RANKS, (1 - q) * n_tok:(2 - q) * n_tok] = none
                rows.append(jnp.where(mask, gate[e][:, lanes], 0.0))
            rows.append(jnp.zeros((yb.shape[2] - n_local * RANKS, n_tok), jnp.float32))
            spread = jnp.concatenate(rows, axis=0).T
            for k, piece in enumerate(split3(spread)):
                gpart[b, q, k] = piece

    def gather(p):
        for k in range(3):
            cols = pl.ds(k * (model // 3), model // 3)
            xg = xall[p, :, :, cols].reshape(2 * n_tok, model // 3)
            xs[:n_local * PAD, cols] = jnp.dot(sel[...], xg, preferred_element_type=jnp.float32).astype(jnp.bfloat16)

    def up(e):
        xr = xs[e * PAD:e * PAD + 2 * PAD, :]
        act = jnp.dot(xr, w1[e], preferred_element_type=jnp.float32)
        lin = jnp.dot(xr, w3[e], preferred_element_type=jnp.float32)
        return (jax.nn.silu(act) * lin).astype(jnp.bfloat16)

    def down(e, b, h):
        yr = jnp.dot(h, w2[e], preferred_element_type=jnp.float32)
        for q in range(2):
            yb[b, q, e * RANKS:(e + 1) * RANKS, :] = yr[q * RANKS:(q + 1) * RANKS].astype(jnp.bfloat16)

    def ffn(b, fresh=False, hooks={}):
        def ready(e):
            if fresh:
                for cp in weight_copies(e):
                    cp.wait()
            return up(e)

        h = None if fresh else up(0)
        for e in range(n_local):
            if fresh:
                h, ahead = ready(e), None
            else:
                ahead = up(e + 1) if e + 1 < n_local else None
            down(e, b, h)
            h = ahead
            for hook in hooks.get(e, ()):
                hook()

    q_copies = {(p, h): remote(pother.at[p, h], qrecv.at[p, h], qsem_s.at[2 * p + h], qsem_r.at[2 * p + h], partner)
                for p in range(4) for h in range(2)}

    def combine(p, b, h):
        for q in (1, 0):
            ycols = yb[b, q, :, h * half:(h + 1) * half]
            acc = jnp.dot(gpart[b, q, 2], ycols, preferred_element_type=jnp.float32)
            acc = acc + jnp.dot(gpart[b, q, 1], ycols, preferred_element_type=jnp.float32)
            acc = acc + jnp.dot(gpart[b, q, 0], ycols, preferred_element_type=jnp.float32)
            if q == 1:
                pother[p, h] = acc
                q_copies[p, h].start()
            else:
                pmine[p, h] = acc

    def chip_sum(p, h):
        q_copies[p, h].wait_recv()
        pmine[p, h] = pmine[p, h] + qrecv[p, h]

    returns = {"to_first": (FIRST, 0, 0, first), "to_second": (SECOND, 1, 1, second),
               "diag_first": (DIAG, 0, 2, first), "diag_second": (DIAG, 1, 3, second),
               "last_second": (SECOND, 0, 4, second), "last_first": (FIRST, 1, 5, first)}
    ret = {name: [remote(pmine.at[p, h, pl.ds(k * hr, hr)], rbuf.at[slot, pl.ds(k * hr, hr)],
                         rsend.at[slot, k], rrecv.at[slot, k], to) for k in range(2)]
           for name, (p, h, slot, to) in returns.items()}

    def start_both(name):
        for cp in ret[name]:
            cp.start()

    def sum_and_send(p, h, name):
        def run():
            chip_sum(p, h)
            start_both(name)
        return run

    def on_first(i):
        if i == 0:
            m_hop[1].wait_recv()
            m_hop[4].start()
            m_hop[3].start()
        x_hop[1][i].wait_recv()
        x_hop[4][i].start()
        if i < CUTS - 1:
            @pl.when(c == 0)
            def _():
                x_hop[3][i].start()
        if i > 0:
            @pl.when(c == 1)
            def _():
                x_hop[3][i - 1].start()
        if i == CUTS - 1:
            x_hop[3][i].start()

    def on_diag(i):
        if i == 0:
            m_hop[3].wait_recv()
            m_hop[5].start()
        x_hop[3][i].wait_recv()
        x_hop[5][i].start()

    def on_second():
        m_hop[2].wait_recv()
        m_hop[6].start()
        wait_x(2)
        start_x(6)

    def after_three():
        on_first(2)
        m_hop[4].wait_recv()
        route(FIRST, 0)
        on_first(3)
        start_x(2)

    m_hop[0].wait_recv()
    route(OWN, 1)
    wait_x(0)
    gather(OWN)
    ffn(1, True, {1: (lambda: on_first(0),), 2: (lambda: on_first(1),), 3: (after_three,)})

    wait_x(4)
    gather(FIRST)
    ffn(0, False, {2: (lambda: on_diag(0), lambda: on_diag(1),), 3: (lambda: on_diag(2), lambda: on_diag(3),)})
    combine(FIRST, 0, 0)

    m_hop[5].wait_recv()
    route(DIAG, 2)
    wait_x(5)
    gather(DIAG)
    ffn(2, False, {0: (sum_and_send(FIRST, 0, "to_first"),)})
    combine(DIAG, 2, 0)
    combine(DIAG, 2, 1)
    combine(FIRST, 0, 1)

    on_second()
    m_hop[6].wait_recv()
    route(SECOND, 0)
    sum_and_send(DIAG, 0, "diag_first")()
    sum_and_send(DIAG, 1, "diag_second")()
    wait_x(6)
    gather(SECOND)
    ffn(0, False, {1: (lambda: chip_sum(FIRST, 1),)})
    combine(SECOND, 0, 1)
    combine(SECOND, 0, 0)
    combine(OWN, 1, 0)
    sum_and_send(SECOND, 1, "to_second")()
    combine(OWN, 1, 1)
    chip_sum(SECOND, 0)

    for k in range(2):
        rows = pl.ds(k * hr, hr)
        ret["diag_second"][k].wait_recv()
        pmine[FIRST, 1, rows, :] = pmine[FIRST, 1, rows, :] + rbuf[3, rows, :]
        ret["last_first"][k].start()
        ret["diag_first"][k].wait_recv()
        pmine[SECOND, 0, rows, :] = pmine[SECOND, 0, rows, :] + rbuf[2, rows, :]
        ret["last_second"][k].start()
    chip_sum(OWN, 0)
    chip_sum(OWN, 1)
    for h, name in ((0, "to_first"), (1, "to_second")):
        for cp in ret[name]:
            cp.wait_recv()
        cols = pl.ds(h * half, half)
        pmine[OWN, h] = (pmine[OWN, h] + xall[OWN, 0, :, cols].astype(jnp.float32)) + rbuf[h]
    for k in range(2):
        rows = pl.ds(k * hr, hr)
        ret["last_first"][k].wait_recv()
        out_ref[rows, half:] = (pmine[OWN, 1, rows, :] + rbuf[5, rows, :]).astype(jnp.bfloat16)
        ret["last_second"][k].wait_recv()
        out_ref[rows, :half] = (pmine[OWN, 0, rows, :] + rbuf[4, rows, :]).astype(jnp.bfloat16)
    for cp in m_hop + [cp for pair in x_hop for cp in pair] + list(q_copies.values()):
        cp.wait_send()
    for pair in ret.values():
        for cp in pair:
            cp.wait_send()


def solution(mesh):
    row_spec = P(('dp', 'ep2', 'ep'), None)
    weight_spec = P(('ep2', 'ep'), None, None)

    def device_step(tokens, expert_ids, gates, w_gate, w_up, w_down):
        n_tok, model = tokens.shape
        n_local, _, ffn = w_gate.shape
        n_top = expert_ids.shape[1]
        half = model // 2
        bf16, f32 = jnp.bfloat16, jnp.float32
        dma = pltpu.SemaphoreType.DMA
        any_spec = pl.BlockSpec(memory_space=pl.ANY)
        return pl.pallas_call(
            layer_kernel,
            out_shape=pltpu.MemorySpace.VMEM((n_tok, model), bf16),
            in_specs=[any_spec] * 6,
            out_specs=pl.BlockSpec(memory_space=pltpu.VMEM),
            scratch_shapes=[
                pltpu.VMEM((4, 2, n_tok, model), bf16),
                pltpu.VMEM((4, 2, 16, n_tok), f32),
                pltpu.VMEM((n_top, n_tok), jnp.int32),
                pltpu.VMEM((n_local, model, ffn), bf16),
                pltpu.VMEM((n_local, model, ffn), bf16),
                pltpu.VMEM((n_local, ffn, model), bf16),
                pltpu.VMEM((n_local * PAD, 2 * n_tok), bf16),
                pltpu.VMEM((3, 2, 3, n_tok, 8 * RANKS), bf16),
                pltpu.VMEM(((n_local + 1) * PAD, model), bf16),
                pltpu.VMEM((3, 2, 8 * RANKS, model), bf16),
                pltpu.VMEM((4, 2, n_tok, half), f32),
                pltpu.VMEM((4, 2, n_tok, half), f32),
                pltpu.VMEM((4, 2, n_tok, half), f32),
                pltpu.VMEM((6, n_tok, half), f32),
                dma((3,)), dma((3, n_local)),
                dma((7,)), dma((7,)),
                dma((7, CUTS)), dma((7, CUTS)),
                dma((8,)), dma((8,)),
                dma((6, 2)), dma((6, 2)),
            ],
            compiler_params=pltpu.CompilerParams(
                collective_id=0, has_side_effects=True, vmem_limit_bytes=60 * 1024 * 1024),
        )(tokens, expert_ids.T, gates.T, w_gate, w_up, w_down)

    return jax.shard_map(device_step, mesh=mesh, in_specs=(row_spec, row_spec, row_spec, weight_spec, weight_spec, weight_spec), out_specs=row_spec, check_vma=False)
```
